128 devices in a mesh: rep: 32 (over z, x, y_hi), tp: 4 (over y_lo, core).
Axes of the slice: x: 4, y: 4 (y_hi: 2, y_lo: 2; y = y_hi * 2 + y_lo), z: 4, core: 2. Of those that a mesh axis runs over, the one named last changes fastest.
Arguments:
- weight: bfloat16 [32, 2048, 7168], P('rep', None, 'tp'), may hold values from -6 to 6
- tokens: bfloat16 [32, 2, 512, 2048], P('rep'), may hold values from -6 to 6
- cotangent: bfloat16 [32, 2, 512, 7168], P('rep', None, None, 'tp'), may hold values from -6 to 6
- batch_order: int32 [32, 2], P('rep'), may hold values from 0 to 1, each once within a row
- step_index: int32 [1], replicated, may hold values from 0 to 999
Outputs:
- averaged: bfloat16 [32, 2048, 7168], P('rep', None, 'tp')
- losses: float32 [32, 2], P('rep')
The draws below stay inside these ranges and needn't reach their ends.
Inputs may be any that keep to these rules, and one draw needn't show every extreme that they name: `batch_order`: each row lists 0 to 1 once.
All inputs are finite; a program needn't handle non-finite values.
Results may differ from the reference program's by a relative error of at most 0.009.
Values may be sent and summed in bfloat16 or wider, within the bound.
A program may use at most 256 MiB of HBM per device.

```python
import jax
import jax.numpy as jnp
from jax import lax

D = 2048
FF = 7168
TOK = 512
STEPS = 2
REPLICAS = 32
N_REP = 32


def steps_of(key, extent, shards, least, largest):
    def one(axis_at, blocks):
        draws = jax.random.uniform(jax.random.fold_in(jax.random.fold_in(key, 6), axis_at), (blocks,), jnp.float32, least / len(shards), largest / len(shards))
        return jnp.repeat(jnp.exp(draws), extent[axis_at] // blocks).reshape((-1,) + (1,) * (len(extent) - axis_at - 1))

    factor_of = one(*shards[0])
    for cut in shards[1:]:
        factor_of = factor_of * one(*cut)
    return factor_of


def gaussian(key, shape, scale, limit, pieces=(), dtype=jnp.bfloat16):
    result = jax.random.normal(key, shape, jnp.float32) * scale
    if len(pieces) > 0:
        result = steps_of(key, shape, pieces, -0.22, 0.18) * result
    return jnp.clip(result, min=-limit, max=limit).astype(dtype)


def setup_inputs(seed: int = 0) -> dict:
    seeds = jax.random.split(jax.random.key(seed), 6)
    return {
        "weight": gaussian(seeds[0], (REPLICAS, D, FF), 1.0, 6.0, ((0, 32), (2, 4))),
        "tokens": gaussian(seeds[1], (REPLICAS, STEPS, TOK, D), 1.0, 6.0, ((0, 32),)),
        "cotangent": gaussian(seeds[2], (REPLICAS, STEPS, TOK, FF), 1.0, 6.0, ((0, 32), (3, 4))),
        "batch_order": jax.vmap(lambda own: jax.random.permutation(own, STEPS))(jax.random.split(seeds[3], REPLICAS)).reshape((REPLICAS, STEPS)).astype(jnp.int32),
        "step_index": jax.random.randint(seeds[4], (1,), 0, 1000).astype(jnp.int32),
    }


beta_first = 0.9
beta_second = 0.95
learn_rate = 0.05
decay_rate = 0.1
adam_eps = 1e-05
norm_eps = 1e-06

def local_chain(operands):
    weight, tokens, cotangent, order = operands
    width_scale = D ** (-0.5)
    master = weight.astype(jnp.float32)
    moment = jnp.zeros(master.shape, jnp.float32)
    second = jnp.zeros(master.shape, jnp.float32)
    losses = []
    for local_step in range(STEPS):
        chosen = order[local_step].astype(jnp.int32)
        inputs = lax.dynamic_index_in_dim(tokens, chosen, 0, keepdims=False)
        target = lax.dynamic_index_in_dim(cotangent, chosen, 0, keepdims=False).astype(jnp.float32)
        current = master.astype(jnp.bfloat16)
        hidden = jnp.dot(inputs, current, preferred_element_type=jnp.float32) * width_scale
        squares = lax.optimization_barrier(jnp.sum(hidden * hidden, axis=1))
        inner = lax.optimization_barrier(jnp.sum(target * hidden, axis=1))
        radius = jnp.sqrt(squares / FF + norm_eps)
        losses.append(jnp.mean(inner / radius))
        grad_rows = (target / radius[:, None] - hidden * (inner / (FF * radius ** 3))[:, None]) / TOK
        grad_rows = grad_rows.astype(jnp.bfloat16)
        gradient = jnp.dot(inputs.T, grad_rows, preferred_element_type=jnp.float32) * width_scale
        moment = beta_first * moment + (1.0 - beta_first) * gradient
        second = beta_second * second + (1.0 - beta_second) * gradient * gradient
        moment_hat = moment / (1.0 - beta_first ** (local_step + 1))
        second_hat = second / (1.0 - beta_second ** (local_step + 1))
        master = master - learn_rate * (moment_hat / (jnp.sqrt(second_hat) + adam_eps) + decay_rate * master)
    return (master.astype(jnp.bfloat16), jnp.stack(losses))

def reference(weight, tokens, cotangent, batch_order, step_index):
    final_weight, losses = lax.map(local_chain, (weight, tokens, cotangent, batch_order))
    levels = N_REP.bit_length() - 1
    distance = (2 ** (step_index[0] % levels)).astype(jnp.int32)
    peer_weight = jnp.roll(final_weight, distance, axis=0)
    averaged = ((final_weight.astype(jnp.float32) + peer_weight.astype(jnp.float32)) * 0.5).astype(jnp.bfloat16)
    return (averaged, losses)
```

```python
import functools

import jax
import jax.numpy as jnp
from jax import lax
from jax.experimental import pallas as pl
from jax.experimental.pallas import tpu as pltpu
from jax.sharding import PartitionSpec as P

beta_first = 0.9
beta_second = 0.95
learn_rate = 0.05
decay_rate = 0.1
adam_eps = 1e-05
norm_eps = 1e-06

F32 = jnp.float32
BF16 = jnp.bfloat16
MESH = pl.DeviceIdType.MESH
BLOCK = 256
LANES = 128
PARTS = 4


def kernel(
    exponent,
    width,
    order_ref,
    w_hbm,
    tok_hbm,
    cot_hbm,
    out_hbm,
    loss_ref,
    wv,
    tokv,
    cotv,
    hv,
    xt,
    w1,
    gb,
    dv,
    rcv,
    hop1,
    hop2,
    acc_s,
    acc_q,
    av,
    bv,
    stats,
    tok_sem,
    w_sem,
    c_sem,
    out_sem,
    st_send,
    st_recv,
    send_sem,
    recv_sem,
    hop_send,
    hop_recv,
):
    blocks = wv.shape[0]
    depth = wv.shape[1]
    tokens = hv.shape[1]
    quarter = depth // PARTS
    scale = depth ** (-0.5)
    eps = adam_eps / scale
    keep = 1.0 - learn_rate * decay_rate
    reps = lax.axis_size("rep")
    tps = lax.axis_size("tp")
    me = lax.axis_index("rep")
    mine = lax.axis_index("tp")
    dist = 2**exponent
    relayed = exponent in (1, 3)

    def ring(rep, by):
        place = lax.rem(lax.div(rep, dist), 4)
        return rep - dist * place + dist * lax.rem(place + by, 4)

    target = lax.rem(me + dist, reps)
    source = lax.rem(me + reps - dist, reps)
    partners = [{"rep": target}, {"rep": source}]
    if relayed:
        behind = ring(me, 3)
        entry = ring(target, 2)
        enters = lax.rem(ring(me, 2) + reps - dist, reps)
        partners += [{"rep": behind}, {"rep": ring(me, 1)}]
        partners += [{"rep": entry}, {"rep": enters}]
    partners += [{"tp": lax.rem(mine + k, tps)} for k in range(1, tps)]

    barrier = pltpu.get_barrier_semaphore()
    for partner in partners:
        pl.semaphore_signal(barrier, inc=1, device_id=partner, device_id_type=MESH)

    first, second = order_ref[0], order_ref[1]

    def columns(n):
        return pl.ds(pl.multiple_of(n * BLOCK, BLOCK), BLOCK)

    def w_copy(n):
        return pltpu.make_async_copy(w_hbm.at[:, columns(n)], wv.at[n], w_sem.at[n])

    def cotangent(n, chosen, half):
        at = pl.ds(pl.multiple_of(n * BLOCK + half * LANES, LANES), LANES)
        return cotv[chosen, :, at].astype(F32)

    tok_copy = pltpu.make_async_copy(tok_hbm, tokv, tok_sem)
    cot_copy = pltpu.make_async_copy(cot_hbm, cotv, c_sem)
    tok_copy.start()
    w_copy(0).start()
    cot_copy.start()
    w_copy(1).start()
    acc_s[...] = jnp.zeros_like(acc_s)
    acc_q[...] = jnp.zeros_like(acc_q)
    tok_copy.wait()

    def add_stats(n, chosen):
        for half in range(BLOCK // LANES):
            at = slice(half * LANES, (half + 1) * LANES)
            part = hv[n, :, at]
            acc_s[...] += part * part
            acc_q[...] += part * cotangent(n, chosen, half)

    def first_forward(n, carry):
        @pl.when(n + 2 < blocks)
        def _():
            w_copy(n + 2).start()

        w_copy(n).wait()
        hv[n] = jnp.dot(tokv[first], wv[n], preferred_element_type=F32)

        @pl.when(n == 0)
        def _():
            cot_copy.wait()

        add_stats(n, first)
        return carry

    lax.fori_loop(0, blocks, first_forward, 0)
    pl.semaphore_wait(barrier, len(partners))

    def exchange(step, chosen):
        stats[step, mine, 0:1, :] = jnp.sum(acc_s[...].T, axis=0, keepdims=True)
        stats[step, mine, 1:2, :] = jnp.sum(acc_q[...].T, axis=0, keepdims=True)
        copies = []
        for k in range(1, tps):
            copy = pltpu.make_async_remote_copy(
                src_ref=stats.at[step, mine],
                dst_ref=stats.at[step, mine],
                send_sem=st_send.at[step, k - 1],
                recv_sem=st_recv.at[step, k - 1],
                device_id={"tp": lax.rem(mine + k, tps)},
                device_id_type=MESH,
            )
            copy.start()
            copies.append(copy)
        acc_s[...] = jnp.zeros_like(acc_s)
        acc_q[...] = jnp.zeros_like(acc_q)
        for at in range(0, depth, BLOCK):
            xt[at : at + BLOCK, :] = tokv[chosen, :, at : at + BLOCK].T
        for copy in copies:
            copy.wait()
        total = stats[step, 0]
        for k in range(1, tps):
            total = total + stats[step, k]
        squares = total[0:1] * (scale * scale)
        inner = total[1:2] * scale
        radius = jnp.sqrt(squares / width + norm_eps)
        inverse = 1.0 / radius
        loss = jnp.sum(inner * inverse, axis=1, keepdims=True) / tokens
        loss_ref[step : step + 1, :] = jnp.broadcast_to(loss, (1, LANES))
        near = inverse * (1.0 / tokens)
        far = inner * inverse * inverse * inverse * (scale / (width * tokens))
        av[...] = jnp.broadcast_to(near, (LANES, tokens)).T
        bv[...] = jnp.broadcast_to(far, (LANES, tokens)).T

    def make_grad_rows(n, chosen):
        for half in range(BLOCK // LANES):
            at = slice(half * LANES, (half + 1) * LANES)
            rows = cotangent(n, chosen, half) * av[...] - hv[n, :, at] * bv[...]
            gb[:, at] = rows.astype(BF16)

    def first_update(grad):
        return grad / (jnp.abs(grad) + eps)

    exchange(0, first)

    def second_forward(n, carry):
        make_grad_rows(n, first)
        for r in range(depth // BLOCK):
            at = slice(r * BLOCK, (r + 1) * BLOCK)
            inside = slice((r * BLOCK) % quarter, (r * BLOCK) % quarter + BLOCK)
            grad = jnp.dot(xt[at, :], gb[...], preferred_element_type=F32)
            master = keep * wv[n, at, :].astype(F32) - learn_rate * first_update(grad)
            w1[at, :] = master.astype(BF16)
            dv[n, r * BLOCK // quarter, inside, :] = grad.astype(BF16)
        hv[n] = jnp.dot(tokv[second], w1[...], preferred_element_type=F32)
        add_stats(n, second)
        return carry

    lax.fori_loop(0, blocks, second_forward, 0)
    exchange(1, second)

    moment_old = beta_first * (1.0 - beta_first) / (1.0 - beta_first**2)
    moment_new = (1.0 - beta_first) / (1.0 - beta_first**2)
    second_old = beta_second * (1.0 - beta_second) / (1.0 - beta_second**2)
    second_new = (1.0 - beta_second) / (1.0 - beta_second**2)

    def direct(n, q):
        return pltpu.make_async_remote_copy(
            src_ref=dv.at[n, q],
            dst_ref=rcv.at[n, q],
            send_sem=send_sem.at[n, q],
            recv_sem=recv_sem.at[n, q],
            device_id={"rep": target},
            device_id_type=MESH,
        )

    def relay(stage, n):
        src = (dv.at[n, 0], hop1.at[n], hop2.at[n])[stage]
        dst = (hop1.at[n], hop2.at[n], rcv.at[n, 0])[stage]
        return pltpu.make_async_remote_copy(
            src_ref=src,
            dst_ref=dst,
            send_sem=hop_send.at[stage, n],
            recv_sem=recv_sem.at[n, 0] if stage == 2 else hop_recv.at[stage, n],
            device_id={"rep": entry if stage == 0 else behind},
            device_id_type=MESH,
        )

    def final_block(n, carry):
        make_grad_rows(n, second)
        for q in range(PARTS):

            def rows(r, inner_carry):
                inside = pl.ds(pl.multiple_of(r * BLOCK, BLOCK), BLOCK)
                at = pl.ds(pl.multiple_of(q * quarter + r * BLOCK, BLOCK), BLOCK)
                new = jnp.dot(xt[at, :], gb[...], preferred_element_type=F32)
                old = dv[n, q, inside, :].astype(F32)
                master = keep * wv[n, at, :].astype(F32) - learn_rate * first_update(old)
                top = moment_old * old + moment_new * new
                bottom = jnp.sqrt(second_old * old * old + second_new * new * new) + eps
                master = keep * master - learn_rate * (top / bottom)
                dv[n, q, inside, :] = master.astype(BF16)
                return inner_carry

            lax.fori_loop(0, quarter // BLOCK, rows, 0)
            if relayed and q == 0:
                relay(0, n).start()
            else:
                direct(n, q).start()
        return carry

    lax.fori_loop(0, blocks, final_block, 0)

    def out_copy(n, q):
        return pltpu.make_async_copy(
            rcv.at[n, q],
            out_hbm.at[q * quarter : (q + 1) * quarter, columns(n)],
            out_sem.at[n, q],
        )

    def average(n, q):
        for r in range(quarter // BLOCK):
            at = slice(r * BLOCK, (r + 1) * BLOCK)
            both = dv[n, q, at, :].astype(F32) + rcv[n, q, at, :].astype(F32)
            rcv[n, q, at, :] = (both * 0.5).astype(BF16)
        out_copy(n, q).start()

    def receive(k, carry):
        for t in range(PARTS - 1):
            if relayed:
                item = k * (PARTS - 1) + t

                @pl.when(item < blocks)
                def _():
                    relay(0, item).wait_recv()
                    relay(1, item).start()

                @pl.when((item >= blocks) & (item < 2 * blocks))
                def _():
                    relay(1, item - blocks).wait_recv()
                    relay(2, item - blocks).start()

                @pl.when(item >= 2 * blocks)
                def _():
                    relay(2, item - 2 * blocks).wait_recv()
                    average(item - 2 * blocks, 0)

            direct(k, t + 1).wait_recv()
            average(k, t + 1)
        if not relayed:
            direct(k, 0).wait_recv()
            average(k, 0)
        return carry

    lax.fori_loop(0, blocks, receive, 0)

    def finish(n, carry):
        for q in range(PARTS):
            if relayed and q == 0:
                for stage in range(3):
                    relay(stage, n).wait_send()
            else:
                direct(n, q).wait_send()
            out_copy(n, q).wait()
        return carry

    lax.fori_loop(0, blocks, finish, 0)


def run(exponent, weight, tokens, cotangent, order):
    depth, width = weight.shape
    steps, count, _ = tokens.shape
    blocks = width // BLOCK
    tps = lax.axis_size("tp")
    quarter = depth // PARTS
    relayed = exponent in (1, 3)
    hop = (blocks, quarter, BLOCK) if relayed else (1, 16, LANES)
    anywhere = pl.BlockSpec(memory_space=pl.ANY)
    dma = pltpu.SemaphoreType.DMA
    flops = 8 * count * depth * width
    return pl.pallas_call(
        functools.partial(kernel, exponent, width * tps),
        out_shape=(
            jax.ShapeDtypeStruct((depth, width), BF16),
            jax.ShapeDtypeStruct((8, LANES), F32),
        ),
        in_specs=[pl.BlockSpec(memory_space=pltpu.SMEM), anywhere, anywhere, anywhere],
        out_specs=(anywhere, pl.BlockSpec(memory_space=pltpu.VMEM)),
        scratch_shapes=[
            pltpu.VMEM((blocks, depth, BLOCK), BF16),
            pltpu.VMEM((steps, count, depth), BF16),
            pltpu.VMEM((steps, count, width), BF16),
            pltpu.VMEM((blocks, count, BLOCK), F32),
            pltpu.VMEM((depth, count), BF16),
            pltpu.VMEM((depth, BLOCK), BF16),
            pltpu.VMEM((count, BLOCK), BF16),
            pltpu.VMEM((blocks, PARTS, quarter, BLOCK), BF16),
            pltpu.VMEM((blocks, PARTS, quarter, BLOCK), BF16),
            pltpu.VMEM(hop, BF16),
            pltpu.VMEM(hop, BF16),
            pltpu.VMEM((count, LANES), F32),
            pltpu.VMEM((count, LANES), F32),
            pltpu.VMEM((count, LANES), F32),
            pltpu.VMEM((count, LANES), F32),
            pltpu.VMEM((steps, tps, 8, count), F32),
            dma,
            dma((blocks,)),
            dma,
            dma((blocks, PARTS)),
            dma((steps, tps - 1)),
            dma((steps, tps - 1)),
            dma((blocks, PARTS)),
            dma((blocks, PARTS)),
            dma((3, blocks)),
            dma((2, blocks)),
        ],
        compiler_params=pltpu.CompilerParams(
            collective_id=exponent + 1,
            has_side_effects=True,
            vmem_limit_bytes=60 * 1024 * 1024,
        ),
        cost_estimate=pl.CostEstimate(
            flops=flops, bytes_accessed=4 * depth * width, transcendentals=0
        ),
        name=f"local_steps_{exponent}",
    )(order, weight, tokens, cotangent)


def shards(weight, tokens, cotangent, batch_order, step_index):
    levels = lax.axis_size("rep").bit_length() - 1
    level = step_index[0] % levels

    def branch(exponent):
        return lambda: run(exponent, weight[0], tokens[0], cotangent[0], batch_order[0])

    averaged, losses = lax.switch(level, [branch(exponent) for exponent in range(levels)])
    return (averaged[None], losses[: tokens.shape[1], 0][None])


def solution(mesh):
    placed = (
        P("rep", None, "tp"),
        P("rep", None, None, None),
        P("rep", None, None, "tp"),
        P("rep", None),
        P(),
    )
    return jax.shard_map(
        shards,
        mesh=mesh,
        in_specs=placed,
        out_specs=(P("rep", None, "tp"), P("rep", None)),
        check_vma=False,
    )
```

```python
import functools

import jax
import jax.numpy as jnp
from jax import lax
from jax.experimental import pallas as pl
from jax.experimental.pallas import tpu as pltpu
from jax.sharding import PartitionSpec as P

beta_first = 0.9
beta_second = 0.95
learn_rate = 0.05
decay_rate = 0.1
adam_eps = 1e-05
norm_eps = 1e-06

F32 = jnp.float32
BF16 = jnp.bfloat16
MESH = pl.DeviceIdType.MESH
BLOCK = 256
LANES = 128
PARTS = 4


def kernel(
    exponent,
    width,
    order_hbm,
    w_hbm,
    tok_hbm,
    cot_hbm,
    out_ref,
    loss_ref,
    wv,
    tokv,
    cotv,
    hv,
    xt,
    w1,
    gb,
    dv,
    rcv,
    hop1,
    hop2,
    acc_s,
    acc_q,
    av,
    bv,
    stats,
    order_ref,
    order_sem,
    tok_sem,
    w_sem,
    c_sem,
    st_send,
    st_recv,
    send_sem,
    recv_sem,
    hop_send,
    hop_recv,
):
    blocks = wv.shape[0]
    depth = wv.shape[1]
    tokens = hv.shape[1]
    quarter = depth // PARTS
    scale = depth ** (-0.5)
    eps = adam_eps / scale
    keep = 1.0 - learn_rate * decay_rate
    reps = lax.axis_size("rep")
    tps = lax.axis_size("tp")
    me = lax.axis_index("rep")
    mine = lax.axis_index("tp")
    dist = 2**exponent
    relayed = exponent in (1, 3)

    def ring(rep, by):
        place = lax.rem(lax.div(rep, dist), 4)
        return rep - dist * place + dist * lax.rem(place + by, 4)

    target = lax.rem(me + dist, reps)
    source = lax.rem(me + reps - dist, reps)
    partners = [{"rep": target}, {"rep": source}]
    if relayed:
        behind = ring(me, 3)
        entry = ring(target, 2)
        enters = lax.rem(ring(me, 2) + reps - dist, reps)
        partners += [{"rep": behind}, {"rep": ring(me, 1)}]
        partners += [{"rep": entry}, {"rep": enters}]
    partners += [{"tp": lax.rem(mine + k, tps)} for k in range(1, tps)]

    barrier = pltpu.get_barrier_semaphore()
    for partner in partners:
        pl.semaphore_signal(barrier, inc=1, device_id=partner, device_id_type=MESH)

    order_copy = pltpu.make_async_copy(order_hbm, order_ref, order_sem)
    order_copy.start()

    def columns(n):
        return pl.ds(pl.multiple_of(n * BLOCK, BLOCK), BLOCK)

    def w_copy(n):
        return pltpu.make_async_copy(w_hbm.at[:, columns(n)], wv.at[n], w_sem.at[n])

    def cotangent(n, chosen, half):
        at = pl.ds(pl.multiple_of(n * BLOCK + half * LANES, LANES), LANES)
        return cotv[chosen, :, at].astype(F32)

    tok_copy = pltpu.make_async_copy(tok_hbm, tokv, tok_sem)
    cot_copy = pltpu.make_async_copy(cot_hbm, cotv, c_sem)
    tok_copy.start()
    w_copy(0).start()
    w_copy(1).start()
    acc_s[...] = jnp.zeros_like(acc_s)
    acc_q[...] = jnp.zeros_like(acc_q)
    order_copy.wait()
    first, second = order_ref[0], order_ref[1]
    tok_copy.wait()
    cot_copy.start()

    def add_stats(hidden, n, chosen):
        hv[n] = hidden
        for half in range(BLOCK // LANES):
            at = slice(half * LANES, (half + 1) * LANES)
            part = hidden[:, at]
            acc_s[...] += part * part
            acc_q[...] += part * cotangent(n, chosen, half)

    def first_forward(n, carry):
        @pl.when(n + 2 < blocks)
        def _():
            w_copy(n + 2).start()

        w_copy(n).wait()
        add_stats(jnp.dot(tokv[first], wv[n], preferred_element_type=F32), n, first)
        return carry

    w_copy(2).start()
    w_copy(0).wait()
    hv[0] = jnp.dot(tokv[first], wv[0], preferred_element_type=F32)
    cot_copy.wait()
    add_stats(hv[0], 0, first)
    lax.fori_loop(1, blocks, first_forward, 0)
    pl.semaphore_wait(barrier, len(partners))

    def exchange(step, chosen):
        stats[step, mine, 0:1, :] = jnp.sum(acc_s[...].T, axis=0, keepdims=True)
        stats[step, mine, 1:2, :] = jnp.sum(acc_q[...].T, axis=0, keepdims=True)
        copies = []
        for k in range(1, tps):
            copy = pltpu.make_async_remote_copy(
                src_ref=stats.at[step, mine],
                dst_ref=stats.at[step, mine],
                send_sem=st_send.at[step, k - 1],
                recv_sem=st_recv.at[step, k - 1],
                device_id={"tp": lax.rem(mine + k, tps)},
                device_id_type=MESH,
            )
            copy.start()
            copies.append(copy)
        acc_s[...] = jnp.zeros_like(acc_s)
        acc_q[...] = jnp.zeros_like(acc_q)
        for at in range(0, depth, BLOCK):
            xt[at : at + BLOCK, :] = tokv[chosen, :, at : at + BLOCK].T
        for copy in copies:
            copy.wait()
        total = stats[step, 0]
        for k in range(1, tps):
            total = total + stats[step, k]
        squares = total[0:1] * (scale * scale)
        inner = total[1:2] * scale
        radius = jnp.sqrt(squares / width + norm_eps)
        inverse = 1.0 / radius
        loss = jnp.sum(inner * inverse, axis=1, keepdims=True) / tokens
        loss_ref[step : step + 1, :] = jnp.broadcast_to(loss, (1, LANES))
        near = inverse * (1.0 / tokens)
        far = inner * inverse * inverse * inverse * (scale / (width * tokens))
        av[...] = jnp.broadcast_to(near, (LANES, tokens)).T
        bv[...] = jnp.broadcast_to(far, (LANES, tokens)).T

    def make_grad_rows(n, chosen):
        for half in range(BLOCK // LANES):
            at = slice(half * LANES, (half + 1) * LANES)
            rows = cotangent(n, chosen, half) * av[...] - hv[n, :, at] * bv[...]
            gb[:, at] = rows.astype(BF16)

    def first_update(grad):
        return grad / (jnp.abs(grad) + eps)

    exchange(0, first)
    make_grad_rows(0, first)

    def second_forward(n, carry):
        for r in range(depth // BLOCK):
            at = slice(r * BLOCK, (r + 1) * BLOCK)
            inside = slice((r * BLOCK) % quarter, (r * BLOCK) % quarter + BLOCK)
            grad = jnp.dot(xt[at, :], gb[...], preferred_element_type=F32)
            master = keep * wv[n, at, :].astype(F32) - learn_rate * first_update(grad)
            w1[at, :] = master.astype(BF16)
            dv[n, r * BLOCK // quarter, inside, :] = grad.astype(BF16)
        make_grad_rows(jnp.minimum(n + 1, blocks - 1), first)
        add_stats(jnp.dot(tokv[second], w1[...], preferred_element_type=F32), n, second)
        return carry

    lax.fori_loop(0, blocks, second_forward, 0)
    exchange(1, second)

    moment_old = beta_first * (1.0 - beta_first) / (1.0 - beta_first**2)
    moment_new = (1.0 - beta_first) / (1.0 - beta_first**2)
    second_old = beta_second * (1.0 - beta_second) / (1.0 - beta_second**2)
    second_new = (1.0 - beta_second) / (1.0 - beta_second**2)

    def direct(n, q):
        return pltpu.make_async_remote_copy(
            src_ref=dv.at[n, q],
            dst_ref=rcv.at[n, q],
            send_sem=send_sem.at[n, q],
            recv_sem=recv_sem.at[n, q],
            device_id={"rep": target},
            device_id_type=MESH,
        )

    def relay(stage, n):
        src = (dv.at[n, 0], hop1.at[n], hop2.at[n])[stage]
        dst = (hop1.at[n], hop2.at[n], rcv.at[n, 0])[stage]
        return pltpu.make_async_remote_copy(
            src_ref=src,
            dst_ref=dst,
            send_sem=hop_send.at[stage, n],
            recv_sem=recv_sem.at[n, 0] if stage == 2 else hop_recv.at[stage, n],
            device_id={"rep": entry if stage == 0 else behind},
            device_id_type=MESH,
        )

    def final_block(n, carry):
        make_grad_rows(n, second)

        def part(q, part_carry):
            def rows(r, inner_carry):
                inside = pl.ds(pl.multiple_of(r * BLOCK, BLOCK), BLOCK)
                at = pl.ds(pl.multiple_of(q * quarter + r * BLOCK, BLOCK), BLOCK)
                new = jnp.dot(xt[at, :], gb[...], preferred_element_type=F32)
                old = dv[n, q, inside, :].astype(F32)
                master = keep * wv[n, at, :].astype(F32) - learn_rate * first_update(old)
                top = moment_old * old + moment_new * new
                bottom = jnp.sqrt(second_old * old * old + second_new * new * new) + eps
                master = keep * master - learn_rate * (top / bottom)
                dv[n, q, inside, :] = master.astype(BF16)
                return inner_carry

            lax.fori_loop(0, quarter // BLOCK, rows, 0)
            if relayed:

                @pl.when(q == 0)
                def _():
                    relay(0, n).start()

                @pl.when(q > 0)
                def _():
                    direct(n, q).start()

            else:
                direct(n, q).start()
            return part_carry

        lax.fori_loop(0, PARTS, part, 0)
        return carry

    lax.fori_loop(0, blocks, final_block, 0)

    def average(n, q):
        for r in range(quarter // BLOCK):
            at = slice(r * BLOCK, (r + 1) * BLOCK)
            both = dv[n, q, at, :].astype(F32) + rcv[n, q, at, :].astype(F32)
            out_ref[q * quarter + r * BLOCK : q * quarter + (r + 1) * BLOCK, columns(n)] = (
                both * 0.5
            ).astype(BF16)

    def receive(k, carry):
        for t in range(PARTS - 1):
            if relayed:
                item = k * (PARTS - 1) + t

                @pl.when(item < blocks)
                def _():
                    relay(0, item).wait_recv()
                    relay(1, item).start()

                @pl.when((item >= blocks) & (item < 2 * blocks))
                def _():
                    relay(1, item - blocks).wait_recv()
                    relay(2, item - blocks).start()

                @pl.when(item >= 2 * blocks)
                def _():
                    relay(2, item - 2 * blocks).wait_recv()
                    average(item - 2 * blocks, 0)

            direct(k, t + 1).wait_recv()
            average(k, t + 1)
        if not relayed:
            direct(k, 0).wait_recv()
            average(k, 0)
        return carry

    lax.fori_loop(0, blocks, receive, 0)

    def finish(n, carry):
        for q in range(PARTS):
            if relayed and q == 0:
                for stage in range(3):
                    relay(stage, n).wait_send()
            else:
                direct(n, q).wait_send()
        return carry

    lax.fori_loop(0, blocks, finish, 0)


def run(exponent, weight, tokens, cotangent, order):
    depth, width = weight.shape
    steps, count, _ = tokens.shape
    blocks = width // BLOCK
    tps = lax.axis_size("tp")
    quarter = depth // PARTS
    relayed = exponent in (1, 3)
    hop = (blocks, quarter, BLOCK) if relayed else (1, 16, LANES)
    anywhere = pl.BlockSpec(memory_space=pl.ANY)
    dma = pltpu.SemaphoreType.DMA
    flops = 8 * count * depth * width
    return pl.pallas_call(
        functools.partial(kernel, exponent, width * tps),
        out_shape=(
            pltpu.VMEM((depth, width), BF16),
            jax.ShapeDtypeStruct((8, LANES), F32),
        ),
        in_specs=[anywhere] * 4,
        out_specs=(pl.BlockSpec(memory_space=pltpu.VMEM),) * 2,
        scratch_shapes=[
            pltpu.VMEM((blocks, depth, BLOCK), BF16),
            pltpu.VMEM((steps, count, depth), BF16),
            pltpu.VMEM((steps, count, width), BF16),
            pltpu.VMEM((blocks, count, BLOCK), F32),
            pltpu.VMEM((depth, count), BF16),
            pltpu.VMEM((depth, BLOCK), BF16),
            pltpu.VMEM((count, BLOCK), BF16),
            pltpu.VMEM((blocks, PARTS, quarter, BLOCK), BF16),
            pltpu.VMEM((blocks, PARTS, quarter, BLOCK), BF16),
            pltpu.VMEM(hop, BF16),
            pltpu.VMEM(hop, BF16),
            pltpu.VMEM((count, LANES), F32),
            pltpu.VMEM((count, LANES), F32),
            pltpu.VMEM((count, LANES), F32),
            pltpu.VMEM((count, LANES), F32),
            pltpu.VMEM((steps, tps, 8, count), F32),
            pltpu.SMEM((steps,), jnp.int32),
            dma,
            dma,
            dma((blocks,)),
            dma,
            dma((steps, tps - 1)),
            dma((steps, tps - 1)),
            dma((blocks, PARTS)),
            dma((blocks, PARTS)),
            dma((3, blocks)),
            dma((2, blocks)),
        ],
        compiler_params=pltpu.CompilerParams(
            collective_id=exponent + 1,
            has_side_effects=True,
            vmem_limit_bytes=48 * 1024 * 1024,
        ),
        cost_estimate=pl.CostEstimate(
            flops=flops, bytes_accessed=4 * depth * width, transcendentals=0
        ),
        name=f"local_steps_{exponent}",
    )(order, weight, tokens, cotangent)


def shards(weight, tokens, cotangent, batch_order, step_index):
    levels = lax.axis_size("rep").bit_length() - 1
    level = step_index[0] % levels

    def branch(exponent):
        return lambda: run(exponent, weight[0], tokens[0], cotangent[0], batch_order[0])

    averaged, losses = lax.switch(level, [branch(exponent) for exponent in range(levels)])
    return (averaged[None], losses[: tokens.shape[1], 0][None])


def solution(mesh):
    placed = (
        P("rep", None, "tp"),
        P("rep", None, None, None),
        P("rep", None, None, "tp"),
        P("rep", None),
        P(),
    )
    return jax.shard_map(
        shards,
        mesh=mesh,
        in_specs=placed,
        out_specs=(P("rep", None, "tp"), P("rep", None)),
        check_vma=False,
    )
```

```python
import functools

import jax
import jax.numpy as jnp
from jax import lax
from jax.experimental import pallas as pl
from jax.experimental.pallas import tpu as pltpu
from jax.sharding import PartitionSpec as P

beta_first = 0.9
beta_second = 0.95
learn_rate = 0.05
decay_rate = 0.1
adam_eps = 1e-05
norm_eps = 1e-06

F32 = jnp.float32
BF16 = jnp.bfloat16
MESH = pl.DeviceIdType.MESH
BLOCK = 256
LANES = 128
PARTS = 4
AHEAD = 2


def kernel(
    exponent,
    width,
    order_hbm,
    w_hbm,
    tok_hbm,
    cot_hbm,
    out_ref,
    loss_ref,
    wv,
    tokv,
    cotv,
    hv,
    xt,
    w1,
    gb,
    dv,
    rcv,
    hop1,
    hop2,
    acc_s,
    acc_q,
    av,
    bv,
    stats,
    order_ref,
    order_sem,
    tok_sem,
    w_sem,
    c_sem,
    st_send,
    st_recv,
    send_sem,
    recv_sem,
    hop_send,
    hop_recv,
):
    blocks = wv.shape[0]
    depth = wv.shape[1]
    tokens = hv.shape[1]
    quarter = depth // PARTS
    scale = depth ** (-0.5)
    eps = adam_eps / scale
    keep = 1.0 - learn_rate * decay_rate
    reps = lax.axis_size("rep")
    tps = lax.axis_size("tp")
    me = lax.axis_index("rep")
    mine = lax.axis_index("tp")
    dist = 2**exponent
    relayed = exponent in (1, 3)

    def ring(rep, by):
        place = lax.rem(lax.div(rep, dist), 4)
        return rep - dist * place + dist * lax.rem(place + by, 4)

    target = lax.rem(me + dist, reps)
    source = lax.rem(me + reps - dist, reps)
    partners = [{"rep": target}, {"rep": source}]
    if relayed:
        behind = ring(me, 3)
        entry = ring(target, 2)
        enters = lax.rem(ring(me, 2) + reps - dist, reps)
        partners += [{"rep": behind}, {"rep": ring(me, 1)}]
        partners += [{"rep": entry}, {"rep": enters}]
    partners += [{"tp": lax.rem(mine + k, tps)} for k in range(1, tps)]

    barrier = pltpu.get_barrier_semaphore()
    for partner in partners:
        pl.semaphore_signal(barrier, inc=1, device_id=partner, device_id_type=MESH)

    order_copy = pltpu.make_async_copy(order_hbm, order_ref, order_sem)
    order_copy.start()

    def columns(n):
        return pl.ds(pl.multiple_of(n * BLOCK, BLOCK), BLOCK)

    def w_copy(n):
        return pltpu.make_async_copy(w_hbm.at[:, columns(n)], wv.at[n], w_sem.at[n])

    def cotangent(n, chosen, half):
        at = pl.ds(pl.multiple_of(n * BLOCK + half * LANES, LANES), LANES)
        return cotv[chosen, :, at].astype(F32)

    tok_copy = pltpu.make_async_copy(tok_hbm, tokv, tok_sem)
    cot_copy = pltpu.make_async_copy(cot_hbm, cotv, c_sem)
    tok_copy.start()
    w_copy(0).start()
    w_copy(1).start()
    acc_s[...] = jnp.zeros_like(acc_s)
    acc_q[...] = jnp.zeros_like(acc_q)
    order_copy.wait()
    first, second = order_ref[0], order_ref[1]
    tok_copy.wait()
    cot_copy.start()

    def add_stats(hidden, n, chosen):
        hv[n] = hidden
        for half in range(BLOCK // LANES):
            at = slice(half * LANES, (half + 1) * LANES)
            part = hidden[:, at]
            acc_s[...] += part * part
            acc_q[...] += part * cotangent(n, chosen, half)

    def first_forward(n, carry):
        @pl.when(n + 2 < blocks)
        def _():
            w_copy(n + 2).start()

        w_copy(n).wait()
        add_stats(jnp.dot(tokv[first], wv[n], preferred_element_type=F32), n, first)
        return carry

    def only_forward(n, carry):
        w_copy(n + 2).start()
        w_copy(n).wait()
        hv[n] = jnp.dot(tokv[first], wv[n], preferred_element_type=F32)
        return carry

    lax.fori_loop(0, AHEAD, only_forward, 0)
    cot_copy.wait()
    lax.fori_loop(AHEAD, blocks, first_forward, 0)

    def late_stats(n, carry):
        add_stats(hv[n], n, first)
        return carry

    lax.fori_loop(0, AHEAD, late_stats, 0)
    pl.semaphore_wait(barrier, len(partners))

    def exchange(step, chosen):
        stats[step, mine, 0:1, :] = jnp.sum(acc_s[...].T, axis=0, keepdims=True)
        stats[step, mine, 1:2, :] = jnp.sum(acc_q[...].T, axis=0, keepdims=True)
        copies = []
        for k in range(1, tps):
            copy = pltpu.make_async_remote_copy(
                src_ref=stats.at[step, mine],
                dst_ref=stats.at[step, mine],
                send_sem=st_send.at[step, k - 1],
                recv_sem=st_recv.at[step, k - 1],
                device_id={"tp": lax.rem(mine + k, tps)},
                device_id_type=MESH,
            )
            copy.start()
            copies.append(copy)
        acc_s[...] = jnp.zeros_like(acc_s)
        acc_q[...] = jnp.zeros_like(acc_q)
        for at in range(0, depth, BLOCK):
            xt[at : at + BLOCK, :] = tokv[chosen, :, at : at + BLOCK].T
        for copy in copies:
            copy.wait()
        total = stats[step, 0]
        for k in range(1, tps):
            total = total + stats[step, k]
        squares = total[0:1] * (scale * scale)
        inner = total[1:2] * scale
        radius = jnp.sqrt(squares / width + norm_eps)
        inverse = 1.0 / radius
        loss = jnp.sum(inner * inverse, axis=1, keepdims=True) / tokens
        loss_ref[step : step + 1, :] = jnp.broadcast_to(loss, (1, LANES))
        near = inverse * (1.0 / tokens)
        far = inner * inverse * inverse * inverse * (scale / (width * tokens))
        av[...] = jnp.broadcast_to(near, (LANES, tokens)).T
        bv[...] = jnp.broadcast_to(far, (LANES, tokens)).T

    def make_grad_rows(n, chosen):
        for half in range(BLOCK // LANES):
            at = slice(half * LANES, (half + 1) * LANES)
            rows = cotangent(n, chosen, half) * av[...] - hv[n, :, at] * bv[...]
            gb[:, at] = rows.astype(BF16)

    def first_update(grad):
        return grad / (jnp.abs(grad) + eps)

    exchange(0, first)
    make_grad_rows(0, first)

    def second_forward(n, carry):
        for r in range(depth // BLOCK):
            at = slice(r * BLOCK, (r + 1) * BLOCK)
            inside = slice((r * BLOCK) % quarter, (r * BLOCK) % quarter + BLOCK)
            grad = jnp.dot(xt[at, :], gb[...], preferred_element_type=F32)
            master = keep * wv[n, at, :].astype(F32) - learn_rate * first_update(grad)
            w1[at, :] = master.astype(BF16)
            dv[n, r * BLOCK // quarter, inside, :] = grad.astype(BF16)
        make_grad_rows(jnp.minimum(n + 1, blocks - 1), first)
        add_stats(jnp.dot(tokv[second], w1[...], preferred_element_type=F32), n, second)
        return carry

    lax.fori_loop(0, blocks, second_forward, 0)
    exchange(1, second)

    moment_old = beta_first * (1.0 - beta_first) / (1.0 - beta_first**2)
    moment_new = (1.0 - beta_first) / (1.0 - beta_first**2)
    second_old = beta_second * (1.0 - beta_second) / (1.0 - beta_second**2)
    second_new = (1.0 - beta_second) / (1.0 - beta_second**2)

    def direct(n, q):
        return pltpu.make_async_remote_copy(
            src_ref=dv.at[n, q],
            dst_ref=rcv.at[n, q],
            send_sem=send_sem.at[n, q],
            recv_sem=recv_sem.at[n, q],
            device_id={"rep": target},
            device_id_type=MESH,
        )

    def relay(stage, n):
        src = (dv.at[n, 0], hop1.at[n], hop2.at[n])[stage]
        dst = (hop1.at[n], hop2.at[n], rcv.at[n, 0])[stage]
        return pltpu.make_async_remote_copy(
            src_ref=src,
            dst_ref=dst,
            send_sem=hop_send.at[stage, n],
            recv_sem=recv_sem.at[n, 0] if stage == 2 else hop_recv.at[stage, n],
            device_id={"rep": entry if stage == 0 else behind},
            device_id_type=MESH,
        )

    def final_block(n, carry):
        make_grad_rows(n, second)

        def part(q, part_carry):
            def rows(r, inner_carry):
                inside = pl.ds(pl.multiple_of(r * BLOCK, BLOCK), BLOCK)
                at = pl.ds(pl.multiple_of(q * quarter + r * BLOCK, BLOCK), BLOCK)
                new = jnp.dot(xt[at, :], gb[...], preferred_element_type=F32)
                old = dv[n, q, inside, :].astype(F32)
                master = keep * wv[n, at, :].astype(F32) - learn_rate * first_update(old)
                top = moment_old * old + moment_new * new
                bottom = jnp.sqrt(second_old * old * old + second_new * new * new) + eps
                master = keep * master - learn_rate * (top / bottom)
                dv[n, q, inside, :] = master.astype(BF16)
                return inner_carry

            lax.fori_loop(0, quarter // BLOCK, rows, 0)
            if relayed:

                @pl.when(q == 0)
                def _():
                    relay(0, n).start()

                @pl.when(q > 0)
                def _():
                    direct(n, q).start()

            else:
                direct(n, q).start()
            return part_carry

        lax.fori_loop(0, PARTS, part, 0)
        return carry

    lax.fori_loop(0, blocks, final_block, 0)

    def average(n, q):
        for r in range(quarter // BLOCK):
            at = slice(r * BLOCK, (r + 1) * BLOCK)
            both = dv[n, q, at, :].astype(F32) + rcv[n, q, at, :].astype(F32)
            out_ref[q * quarter + r * BLOCK : q * quarter + (r + 1) * BLOCK, columns(n)] = (
                both * 0.5
            ).astype(BF16)

    def receive(k, carry):
        if not relayed:
            direct(k, 0).wait_recv()
            average(k, 0)
        for t in range(PARTS - 1):
            if relayed:
                item = k * (PARTS - 1) + t

                @pl.when(item < blocks)
                def _():
                    relay(0, item).wait_recv()
                    relay(1, item).start()

                @pl.when((item >= blocks) & (item < 2 * blocks))
                def _():
                    relay(1, item - blocks).wait_recv()
                    relay(2, item - blocks).start()

                @pl.when(item >= 2 * blocks)
                def _():
                    relay(2, item - 2 * blocks).wait_recv()
                    average(item - 2 * blocks, 0)

            direct(k, t + 1).wait_recv()
            average(k, t + 1)
        return carry

    lax.fori_loop(0, blocks, receive, 0)

    def finish(n, carry):
        for q in range(PARTS):
            if relayed and q == 0:
                for stage in range(3):
                    relay(stage, n).wait_send()
            else:
                direct(n, q).wait_send()
        return carry

    lax.fori_loop(0, blocks, finish, 0)


def run(exponent, weight, tokens, cotangent, order):
    depth, width = weight.shape
    steps, count, _ = tokens.shape
    blocks = width // BLOCK
    tps = lax.axis_size("tp")
    quarter = depth // PARTS
    relayed = exponent in (1, 3)
    hop = (blocks, quarter, BLOCK) if relayed else (1, 16, LANES)
    anywhere = pl.BlockSpec(memory_space=pl.ANY)
    dma = pltpu.SemaphoreType.DMA
    flops = 8 * count * depth * width
    return pl.pallas_call(
        functools.partial(kernel, exponent, width * tps),
        out_shape=(
            pltpu.VMEM((depth, width), BF16),
            jax.ShapeDtypeStruct((8, LANES), F32),
        ),
        in_specs=[anywhere] * 4,
        out_specs=(pl.BlockSpec(memory_space=pltpu.VMEM),) * 2,
        scratch_shapes=[
            pltpu.VMEM((blocks, depth, BLOCK), BF16),
            pltpu.VMEM((steps, count, depth), BF16),
            pltpu.VMEM((steps, count, width), BF16),
            pltpu.VMEM((blocks, count, BLOCK), F32),
            pltpu.VMEM((depth, count), BF16),
            pltpu.VMEM((depth, BLOCK), BF16),
            pltpu.VMEM((count, BLOCK), BF16),
            pltpu.VMEM((blocks, PARTS, quarter, BLOCK), BF16),
            pltpu.VMEM((blocks, PARTS, quarter, BLOCK), BF16),
            pltpu.VMEM(hop, BF16),
            pltpu.VMEM(hop, BF16),
            pltpu.VMEM((count, LANES), F32),
            pltpu.VMEM((count, LANES), F32),
            pltpu.VMEM((count, LANES), F32),
            pltpu.VMEM((count, LANES), F32),
            pltpu.VMEM((steps, tps, 8, count), F32),
            pltpu.SMEM((steps,), jnp.int32),
            dma,
            dma,
            dma((blocks,)),
            dma,
            dma((steps, tps - 1)),
            dma((steps, tps - 1)),
            dma((blocks, PARTS)),
            dma((blocks, PARTS)),
            dma((3, blocks)),
            dma((2, blocks)),
        ],
        compiler_params=pltpu.CompilerParams(
            collective_id=exponent + 1,
            has_side_effects=True,
            vmem_limit_bytes=48 * 1024 * 1024,
        ),
        cost_estimate=pl.CostEstimate(
            flops=flops, bytes_accessed=4 * depth * width, transcendentals=0
        ),
        name=f"local_steps_{exponent}",
    )(order, weight, tokens, cotangent)


def shards(weight, tokens, cotangent, batch_order, step_index):
    levels = lax.axis_size("rep").bit_length() - 1
    level = step_index[0] % levels

    def branch(exponent):
        return lambda: run(exponent, weight[0], tokens[0], cotangent[0], batch_order[0])

    averaged, losses = lax.switch(level, [branch(exponent) for exponent in range(levels)])
    return (averaged[None], losses[: tokens.shape[1], 0][None])


def solution(mesh):
    placed = (
        P("rep", None, "tp"),
        P("rep", None, None, None),
        P("rep", None, None, "tp"),
        P("rep", None),
        P(),
    )
    return jax.shard_map(
        shards,
        mesh=mesh,
        in_specs=placed,
        out_specs=(P("rep", None, "tp"), P("rep", None)),
        check_vma=False,
    )
```
